32 devices in a mesh: node: 16 (over z, x, core), local: 2 (over y).
Axes of the slice: x: 2, y: 2, z: 4, core: 2. Of those that a mesh axis runs over, the one named last changes fastest.
Arguments:
- hidden: bfloat16 [2, 4096, 4096], P('local', 'node'), may hold values from -6 to 6
- queries: bfloat16 [2, 4096, 2048], P('local', 'node'), may hold values from -30 to 30
- saved_keys: bfloat16 [2, 4096, 512], P('local', 'node'), may hold values from -30 to 30
- grad_out: bfloat16 [2, 4096, 2048], P('local', 'node'), may hold values from -6 to 6
- value_weight: bfloat16 [4096, 512], P('local'), may hold values from -0.09375 to 0.09375
- doc_lengths: int32 [2, 16], P('local'), may hold values from 0 to 1024, as said below
- doc_order: int32 [2, 16], P('local'), may hold values from 0 to 15, each once within a row
Outputs:
- query_grad: bfloat16 [2, 4096, 2048], P('local', 'node')
- key_grad: bfloat16 [2, 4096, 512], P('local', 'node')
- input_grad: bfloat16 [2, 4096, 4096], P('local', 'node')
- weight_grad: float32 [4096, 512], P(('node', 'local'))
The draws below stay inside these ranges and needn't reach their ends.
Inputs may be any that keep to these rules, and one draw needn't show every extreme that they name: `doc_lengths`: a document occupies ceil(length / 256) whole blocks, at most 4; the documents of a sequence fill its 16 blocks exactly; in every sequence some document takes 4 blocks.
All inputs are finite; a program needn't handle non-finite values.
Results may differ from the reference program's by a relative error of at most 0.0085.
Values may be sent and summed in bfloat16 or wider, within the bound.
A program may use at most 128 MiB of HBM per device.

```python
import jax
import jax.numpy as jnp
from jax import lax

D = 4096
HD = 128
KVH = 4
GROUP = 4
BLOCK = 256
DOCB = 4
QW = 2048
KVW = 512
NBLK = 16
SEQLEN = 4096
SEQS = 2


def paired_rows(key):
    base = jax.random.fold_in(key, 17)
    key_query, key_keys = jax.random.split(base)
    query_draw = jnp.clip(jax.random.normal(key_query, (SEQS, SEQLEN, QW), jnp.float32), -6.0, 6.0)
    key_draw = jnp.clip(jax.random.normal(key_keys, (SEQS, SEQLEN, KVW), jnp.float32), -6.0, 6.0)
    return (query_draw, key_draw)


def draw_queries(key, part):
    return paired_rows(key)[0].astype(jnp.bfloat16)


def draw_saved_keys(key, part):
    return paired_rows(key)[1].astype(jnp.bfloat16)


def draw_doc_lengths(key, part):
    key_count, key_len = jax.random.split(jax.random.fold_in(key, 3))
    counts = jax.random.randint(key_count, (SEQS, NBLK), 1, DOCB + 1)
    counts = counts.at[:, 1].set(DOCB)
    ends = jnp.cumsum(counts, axis=1)
    starts = ends - counts
    living = starts < NBLK
    counts = jnp.where(living, jnp.minimum(counts, NBLK - starts), 0)
    extra = jax.random.randint(key_len, (SEQS, NBLK), 1, BLOCK + 1)
    return jnp.where(living, (counts - 1) * BLOCK + extra, 0).astype(jnp.int32)


def strengthened(values, key, source, target, parts, factor):
    def block_of(position):
        return (jnp.arange(values.shape[position]) // (values.shape[position] // parts)).reshape((-1,) + (1,) * (values.ndim - 1 - position))

    near = jax.random.permutation(key, parts)[block_of(target)]
    second = (block_of(target) + parts // 2) % parts
    return jnp.where((block_of(source) == near) | (block_of(source) == second), factor * values, values)


def block_scale(rng, dims, cuts, smallest, largest):
    loudness, own = 1.0, jax.random.fold_in(rng, 6)
    for dim, parts in cuts:
        draws = jnp.exp(jax.random.uniform(jax.random.fold_in(own, dim), (parts,), jnp.float32, smallest / len(cuts), largest / len(cuts)))
        loudness = loudness * jnp.repeat(draws, dims[dim] // parts).reshape([-1 if axis == dim else 1 for axis in range(len(dims))])
    return loudness


def normal_values(stream_key, extent, spread, limit, shards=(), held_as=jnp.bfloat16):
    gain = block_scale(stream_key, extent, shards, -0.22, 0.18) if shards else 1.0
    entries = jax.random.normal(stream_key, extent, jnp.float32) * spread * gain
    return jnp.minimum(jnp.maximum(entries, -limit), limit).astype(held_as)


def gaussian_with(key, shape, deviation, most, cuts, heavy, kind=jnp.bfloat16):
    result = deviation * jax.random.normal(key, shape, jnp.float32)
    if cuts:
        result = result * block_scale(key, shape, cuts, -0.22, 0.18)
    return jnp.clip(strengthened(result, jax.random.fold_in(key, 3), *heavy), -most, most).astype(kind)


def setup_inputs(seed: int = 0) -> dict:
    arg_keys = jax.random.split(jax.random.key(seed), 8)
    hidden = gaussian_with(arg_keys[0], (SEQS, SEQLEN, D), 1.0, 6.0, ((0, 2), (1, 16)), (1, 2, 16, 2.0))
    queries = draw_queries(jax.random.fold_in(arg_keys[7], 71), 0)
    saved_keys = draw_saved_keys(jax.random.fold_in(arg_keys[7], 71), 0)
    grad_out = normal_values(arg_keys[3], (SEQS, SEQLEN, QW), 1.0, 6.0, ((0, 2), (1, 16)))
    value_weight = normal_values(arg_keys[4], (D, KVW), D ** -0.5, 0.09375, ((0, 2),))
    doc_lengths = draw_doc_lengths(jax.random.fold_in(arg_keys[7], 71), 0)
    doc_order = jax.vmap(lambda own: jax.random.permutation(own, NBLK))(jax.random.split(arg_keys[6], SEQS)).reshape((SEQS, NBLK)).astype(jnp.int32)
    return {"hidden": hidden, "queries": queries, "saved_keys": saved_keys, "grad_out": grad_out, "value_weight": value_weight, "doc_lengths": doc_lengths, "doc_order": doc_order}


masked_score = -1e30


def doc_layout(lengths_row, order_row):
    slot_ids = jnp.arange(NBLK, dtype=jnp.int32)
    picked = order_row[:, None] == slot_ids[None, :]
    lens_ord = jnp.sum(jnp.where(picked, lengths_row[None, :], 0), axis=1).astype(jnp.int32)
    block_count = ((lens_ord + BLOCK - 1) // BLOCK).astype(jnp.int32)
    first_block = (jnp.cumsum(block_count) - block_count).astype(jnp.int32)
    return lens_ord, block_count, first_block


def block_info(block_index, lens_ord, block_count, first_block):
    member = (first_block <= block_index) & (block_index < first_block + block_count)
    has_doc = jnp.any(member)
    doc_start = jnp.sum(jnp.where(member, first_block, 0)).astype(jnp.int32)
    length = jnp.sum(jnp.where(member, lens_ord, 0)).astype(jnp.int32)
    return jnp.where(has_doc, doc_start, -1).astype(jnp.int32), length


def window_mask(block_index, layout):
    doc_start, length = block_info(block_index, *layout)
    inside = jnp.arange(BLOCK, dtype=jnp.int32)
    query_ok = (block_index - doc_start) * BLOCK + inside < length
    mask_parts = []
    for offset in range(DOCB - 1, -1, -1):
        other_block = block_index - offset
        other_start, other_len = block_info(other_block, *layout)
        key_ok = (other_start == doc_start) & ((other_block - doc_start) * BLOCK + inside < length)
        allowed = jnp.broadcast_to(key_ok[None, :], (BLOCK, BLOCK))
        if offset == 0:
            allowed = allowed & (inside[None, :] <= inside[:, None])
        mask_parts.append(allowed)
    return query_ok, jnp.concatenate(mask_parts, axis=1)


def tile_grads(query_rows, grad_rows, key_window, value_window, allowed):
    width = key_window.shape[0]
    score_scale = HD ** -0.5
    q_heads = query_rows.reshape(BLOCK, KVH, GROUP, HD).astype(jnp.float32)
    g_heads = grad_rows.reshape(BLOCK, KVH, GROUP, HD).astype(jnp.float32)
    k_heads = key_window.reshape(width, KVH, HD).astype(jnp.float32)
    v_heads = value_window.reshape(width, KVH, HD).astype(jnp.float32)
    scores = jnp.einsum("tgjd,wgd->gjtw", q_heads, k_heads) * score_scale
    scores = jnp.where(allowed[None, None], scores, masked_score)
    peak = jnp.max(scores, axis=3, keepdims=True)
    expd = jnp.exp(scores - peak)
    attn_probs = expd / jnp.sum(expd, axis=3, keepdims=True)
    attn_low = attn_probs.astype(jnp.bfloat16).astype(jnp.float32)
    attn_out = jnp.einsum("gjtw,wgd->tgjd", attn_low, v_heads)
    prob_grad = jnp.einsum("tgjd,wgd->gjtw", g_heads, v_heads)
    row_delta = jnp.einsum("tgjd,tgjd->gjt", g_heads, attn_out)
    score_grad = (attn_probs * (prob_grad - row_delta[..., None]) * score_scale).astype(jnp.bfloat16).astype(jnp.float32)
    query_grad = jnp.einsum("gjtw,wgd->tgjd", score_grad, k_heads).reshape(BLOCK, QW).astype(jnp.bfloat16)
    key_grad = jnp.einsum("gjtw,tgjd->wgd", score_grad, q_heads).reshape(width, KVW)
    value_grad = jnp.einsum("gjtw,tgjd->wgd", attn_low, g_heads).reshape(width, KVW)
    return query_grad, key_grad, value_grad


def gather_window(windows):
    pieces = windows.reshape(NBLK, DOCB, BLOCK, KVW)
    summed = jnp.zeros((NBLK + DOCB - 1, BLOCK, KVW), jnp.float32)
    for offset in range(DOCB):
        summed = summed.at[offset:offset + NBLK].add(pieces[:, offset])
    return summed[DOCB - 1:].reshape(SEQLEN, KVW)


def reference(hidden, queries, saved_keys, grad_out, value_weight, doc_lengths, doc_order):
    flat_hidden = hidden.reshape(SEQS * SEQLEN, D)
    values = jnp.dot(flat_hidden, value_weight, preferred_element_type=jnp.float32).astype(jnp.bfloat16)
    values = values.reshape(SEQS, SEQLEN, KVW)
    query_list, key_list, value_list = [], [], []
    for sequence in range(SEQS):
        layout = doc_layout(doc_lengths[sequence], doc_order[sequence])
        padding = jnp.zeros(((DOCB - 1) * BLOCK, KVW), jnp.bfloat16)
        key_padded = jnp.concatenate([padding, saved_keys[sequence]], axis=0)
        value_padded = jnp.concatenate([padding, values[sequence]], axis=0)
        seq_queries = queries[sequence]
        seq_grads = grad_out[sequence]

        def one_block(block_index):
            query_ok, allowed = window_mask(block_index, layout)
            first_row = (block_index * BLOCK).astype(jnp.int32)
            query_rows = lax.dynamic_slice_in_dim(seq_queries, first_row, BLOCK, 0)
            grad_rows = lax.dynamic_slice_in_dim(seq_grads, first_row, BLOCK, 0)
            grad_rows = grad_rows * query_ok[:, None].astype(grad_rows.dtype)
            key_window = lax.dynamic_slice_in_dim(key_padded, first_row, DOCB * BLOCK, 0)
            value_window = lax.dynamic_slice_in_dim(value_padded, first_row, DOCB * BLOCK, 0)
            return tile_grads(query_rows, grad_rows, key_window, value_window, allowed)

        block_query, block_key, block_value = lax.map(one_block, jnp.arange(NBLK, dtype=jnp.int32))
        query_list.append(block_query.reshape(SEQLEN, QW))
        key_list.append(gather_window(block_key))
        value_list.append(gather_window(block_value))
    query_grad = jnp.stack(query_list)
    key_grad = jnp.stack(key_list).astype(jnp.bfloat16)
    value_low = jnp.stack(value_list).astype(jnp.bfloat16).reshape(SEQS * SEQLEN, KVW)
    input_grad = jnp.dot(value_low, value_weight.T, preferred_element_type=jnp.float32).astype(jnp.bfloat16)
    weight_grad = jnp.dot(flat_hidden.T, value_low, preferred_element_type=jnp.float32)
    return query_grad, key_grad, input_grad.reshape(SEQS, SEQLEN, D), weight_grad
```

```python
import jax
import jax.numpy as jnp
from jax import lax
from jax.experimental import pallas as pl
from jax.experimental.pallas import tpu as pltpu
from jax.sharding import PartitionSpec as P

HD = 128
DOCB = 4
BF16 = jnp.bfloat16
F32 = jnp.float32

masked_score = -1e30


def from_behind(block, axis, distance, parity=None):
    devices = range(lax.axis_size(axis))
    route = [(i - distance, i) for i in devices if i - distance in devices]
    if parity is not None:
        route = [(a, b) for a, b in route if a % 2 == parity]
    return lax.ppermute(block, axis, route)


def swap(block, axis, bit):
    return lax.ppermute(block, axis, [(i, i ^ bit) for i in range(lax.axis_size(axis))])


def doc_layout(lengths_row, order_row, block_rows):
    slot_total = lengths_row.shape[0]
    slot_ids = jnp.arange(slot_total, dtype=jnp.int32)
    picked = order_row[:, None] == slot_ids[None, :]
    lens_ord = jnp.sum(jnp.where(picked, lengths_row[None, :], 0), axis=1)
    block_count = (lens_ord + block_rows - 1) // block_rows
    first_block = jnp.cumsum(block_count) - block_count
    return (lens_ord, block_count, first_block)


def block_info(block_index, lens_ord, block_count, first_block):
    member = (first_block <= block_index) & (block_index < first_block + block_count)
    has_doc = jnp.any(member)
    doc_start = jnp.sum(jnp.where(member, first_block, 0))
    length = jnp.sum(jnp.where(member, lens_ord, 0))
    return (jnp.where(has_doc, doc_start, -1), length)


def window_rows(block_index, layout, block_rows):
    doc_start, length = block_info(block_index, *layout)
    inside = jnp.arange(block_rows, dtype=jnp.int32)
    query_ok = (block_index - doc_start) * block_rows + inside < length
    key_parts = []
    for offset in range(DOCB - 1, -1, -1):
        other_block = block_index - offset
        other_start, _ = block_info(other_block, *layout)
        key_parts.append(
            (other_start == doc_start)
            & ((other_block - doc_start) * block_rows + inside < length)
        )
    return query_ok[:, None], jnp.concatenate(key_parts)[:, None]


def attention_kernel(*refs):
    query_ref, grad_ref, query_ok_ref, key_ok_ref = refs[:4]
    key_refs = refs[4 : 4 + DOCB]
    value_refs = refs[4 + DOCB : 4 + 2 * DOCB]
    query_out = refs[4 + 2 * DOCB]
    pair_outs = refs[5 + 2 * DOCB :]
    rows = query_ref.shape[0]
    group = query_ref.shape[1] // HD
    width = DOCB * rows
    scale = HD ** (-0.5)
    keys = jnp.concatenate([ref[...] for ref in key_refs], axis=0)
    values = jnp.concatenate([ref[...] for ref in value_refs], axis=0)
    keys_turned = keys.T
    key_at = lax.broadcasted_iota(jnp.int32, (width, rows), 0) - (width - rows)
    query_at = lax.broadcasted_iota(jnp.int32, (width, rows), 1)
    allowed = (key_ok_ref[...] > 0.0) & (key_at <= query_at)
    query_ok = query_ok_ref[...]
    contract_last = (((1,), (1,)), ((), ()))
    key_sum = value_sum = None
    for head in range(group):
        cols = slice(head * HD, (head + 1) * HD)
        q = query_ref[:, cols]
        g = grad_ref[:, cols] * query_ok
        scores = lax.dot_general(keys, q, contract_last, preferred_element_type=F32)
        scores = jnp.where(allowed, scores * scale, masked_score)
        expd = jnp.exp(scores - jnp.max(scores, axis=0, keepdims=True))
        probs = expd * (1.0 / jnp.sum(expd, axis=0, keepdims=True))
        probs_low = probs.astype(BF16)
        prob_grad = lax.dot_general(values, g, contract_last, preferred_element_type=F32)
        delta = jnp.sum(probs_low.astype(F32) * prob_grad, axis=0, keepdims=True)
        score_grad = (probs * (prob_grad - delta) * scale).astype(BF16)
        query_grad = jnp.dot(keys_turned, score_grad, preferred_element_type=F32)
        query_out[:, cols] = query_grad.T.astype(BF16)
        key_part = jnp.dot(score_grad, q, preferred_element_type=F32)
        value_part = jnp.dot(probs_low, g, preferred_element_type=F32)
        key_sum = key_part if key_sum is None else key_sum + key_part
        value_sum = value_part if value_sum is None else value_sum + value_part
    for place in range(DOCB):
        part = slice(place * rows, (place + 1) * rows)
        for ref, total in ((pair_outs[2 * place], key_sum), (pair_outs[2 * place + 1], value_sum)):
            ref[...] = total[part].astype(ref.dtype)


def window_grads(query_rows, grad_rows, keys, values, query_ok, key_ok):
    rows, query_cols = query_rows.shape
    kv_cols = keys[0].shape[1]
    heads = kv_cols // HD
    wide = pl.BlockSpec((rows, query_cols // heads), lambda h: (0, h))
    thin = pl.BlockSpec((rows, HD), lambda h: (0, h))
    out_shape = [jax.ShapeDtypeStruct((rows, query_cols), BF16)]
    for place in range(DOCB):
        kind = F32 if place == DOCB - 1 else BF16
        out_shape += [jax.ShapeDtypeStruct((rows, kv_cols), kind)] * 2
    flops = 10 * rows * DOCB * rows * query_cols
    outs = pl.pallas_call(
        attention_kernel,
        grid=(heads,),
        out_shape=out_shape,
        in_specs=[
            wide,
            wide,
            pl.BlockSpec((rows, 1), lambda h: (0, 0)),
            pl.BlockSpec((DOCB * rows, 1), lambda h: (0, 0)),
        ]
        + [thin] * (2 * DOCB),
        out_specs=[wide] + [thin] * (2 * DOCB),
        compiler_params=pltpu.CompilerParams(vmem_limit_bytes=48 * 2**20),
        cost_estimate=pl.CostEstimate(
            flops=flops, bytes_accessed=8 * 2**20, transcendentals=rows * DOCB * rows * query_cols // HD
        ),
    )(query_rows, grad_rows, query_ok, key_ok, *keys, *values)
    return outs[0], [tuple(outs[1 + 2 * p : 3 + 2 * p]) for p in range(DOCB)]


def window_of(block, core):
    two_back = from_behind(block, "node", 2)
    three_back = from_behind(block, "node", 3, parity=1)
    partner = swap(block, "node", 1)
    shared = swap(two_back, "node", 1)
    first = core == 0
    return [
        jnp.where(first, three_back, shared),
        two_back,
        jnp.where(first, shared, partner),
        block,
    ]


def sum_to_owner(pieces, core):
    three, two, one, own = pieces
    first = core == 0
    both = lambda a, b: tuple(jnp.where(first, x, y) for x, y in zip(a, b))
    send_shared = both(one, three)
    shared = [swap(x, "node", 1) for x in send_shared]
    near = [from_behind(x, "node", -1, parity=1) for x in one]
    far = [from_behind(x, "node", -3, parity=0) for x in three]
    paired = [(x.astype(F32) + y.astype(F32)).astype(BF16) for x, y in zip(two, shared)]
    back = [from_behind(x, "node", -2) for x in paired]
    return [
        o + n.astype(F32) + f.astype(F32) + b.astype(F32) for o, n, f, b in zip(own, near, far, back)
    ]


def gather_weight(weight, core):
    count, me = lax.axis_size("local"), lax.axis_index("local")
    rows = weight.shape[0]
    half = lax.dynamic_slice_in_dim(weight, core * (rows // 2), rows // 2, 0)
    pieces = [weight]
    for step in range(1, count):
        got = lax.ppermute(half, "local", [((i + step) % count, i) for i in range(count)])
        other = swap(got, "node", 1)
        pieces += [jnp.where(core == 0, got, other), jnp.where(core == 0, other, got)]
    around = jnp.concatenate(pieces + pieces, axis=0)
    return lax.dynamic_slice_in_dim(around, ((count - me) % count) * rows, count * rows, 0)


def halve(total, dim, axis, bit):
    mine = (lax.axis_index(axis) // bit) % 2
    pick = lambda i: lax.dynamic_index_in_dim(total, i, dim, keepdims=False)
    got = swap(pick(1 - mine).astype(BF16), axis, bit)
    return pick(mine) + got.astype(F32)


def scatter_weight_grad(x_rows, value_low, core):
    nodes, locals_ = lax.axis_size("node"), lax.axis_size("local")
    tokens, width = x_rows.shape
    kv_cols = value_low.shape[1]
    owner_rows = width // (nodes * locals_)
    split = x_rows.reshape(tokens, nodes // 2, 2, locals_ * owner_rows)
    contract_rows = (((0,), (0,)), ((), ()))

    def part(which):
        cols = lax.dynamic_index_in_dim(split, which, 2, keepdims=False)
        return lax.dot_general(
            cols.reshape(tokens, width // 2), value_low, contract_rows, preferred_element_type=F32
        )

    got = swap(part(1 - core).astype(BF16), "node", 1)
    total = part(core) + got.astype(F32)
    node_bits = [("node", 2**b) for b in range(1, nodes.bit_length() - 1)]
    local_bits = [("local", 2**b) for b in range(locals_.bit_length() - 1)]
    dims = node_bits[::-1] + local_bits[::-1]
    orders = (local_bits + node_bits, node_bits[:1] + local_bits + node_bits[1:])
    columns = kv_cols // 2
    done = []
    for which, order in enumerate(orders):
        piece = total[:, which * columns : (which + 1) * columns]
        piece = piece.reshape((2,) * len(dims) + (owner_rows, columns))
        left = list(dims)
        for step in order:
            piece = halve(piece, left.index(step), *step)
            left.remove(step)
        done.append(piece)
    return jnp.concatenate(done, axis=1)


def local(hidden, queries, saved_keys, grad_out, value_weight, doc_lengths, doc_order):
    block_index = lax.axis_index("node")
    core = block_index % 2
    x_rows = hidden[0]
    row_count = x_rows.shape[0]
    full_weight = gather_weight(value_weight, core)
    keys = window_of(saved_keys[0], core)
    layout = doc_layout(doc_lengths[0], doc_order[0], row_count)
    query_ok, key_ok = window_rows(block_index, layout, row_count)
    values = window_of(jnp.dot(x_rows, full_weight, preferred_element_type=F32).astype(BF16), core)
    query_grad, pieces = window_grads(
        queries[0], grad_out[0], keys, values, query_ok.astype(BF16), key_ok.astype(F32)
    )
    key_total, value_total = sum_to_owner(pieces, core)
    value_low = value_total.astype(BF16)
    weight_grad = scatter_weight_grad(x_rows, value_low, core)
    input_grad = lax.dot_general(
        value_low, full_weight, (((1,), (1,)), ((), ())), preferred_element_type=F32
    )
    return (
        query_grad[None],
        key_total.astype(BF16)[None],
        input_grad.astype(BF16)[None],
        weight_grad,
    )


def solution(mesh):
    placed = (
        P("local", "node", None),
        P("local", "node", None),
        P("local", "node", None),
        P("local", "node", None),
        P("local", None),
        P("local", None),
        P("local", None),
    )
    return jax.shard_map(
        local,
        mesh=mesh,
        in_specs=placed,
        out_specs=(
            P("local", "node", None),
            P("local", "node", None),
            P("local", "node", None),
            P(("node", "local"), None),
        ),
        check_vma=False,
    )
```

```python
import jax
import jax.numpy as jnp
from jax import lax
from jax.experimental import pallas as pl
from jax.experimental.pallas import tpu as pltpu
from jax.sharding import PartitionSpec as P

HD = 128
DOCB = 4
BF16 = jnp.bfloat16
F32 = jnp.float32

masked_score = -1e30


def from_behind(block, axis, distance, parity=None):
    devices = range(lax.axis_size(axis))
    route = [(i - distance, i) for i in devices if i - distance in devices]
    if parity is not None:
        route = [(a, b) for a, b in route if a % 2 == parity]
    return lax.ppermute(block, axis, route)


def swap(block, axis, bit):
    return lax.ppermute(block, axis, [(i, i ^ bit) for i in range(lax.axis_size(axis))])


def doc_layout(lengths_row, order_row, block_rows):
    slot_total = lengths_row.shape[0]
    slot_ids = jnp.arange(slot_total, dtype=jnp.int32)
    picked = order_row[:, None] == slot_ids[None, :]
    lens_ord = jnp.sum(jnp.where(picked, lengths_row[None, :], 0), axis=1)
    block_count = (lens_ord + block_rows - 1) // block_rows
    first_block = jnp.cumsum(block_count) - block_count
    return (lens_ord, block_count, first_block)


def block_info(block_index, lens_ord, block_count, first_block):
    member = (first_block <= block_index) & (block_index < first_block + block_count)
    has_doc = jnp.any(member)
    doc_start = jnp.sum(jnp.where(member, first_block, 0))
    length = jnp.sum(jnp.where(member, lens_ord, 0))
    return (jnp.where(has_doc, doc_start, -1), length)


def window_rows(block_index, layout, block_rows):
    doc_start, length = block_info(block_index, *layout)
    inside = jnp.arange(block_rows, dtype=jnp.int32)
    query_ok = (block_index - doc_start) * block_rows + inside < length
    key_parts = []
    for offset in range(DOCB - 1, -1, -1):
        other_block = block_index - offset
        other_start, _ = block_info(other_block, *layout)
        key_parts.append(
            (other_start == doc_start)
            & ((other_block - doc_start) * block_rows + inside < length)
        )
    return query_ok[:, None], jnp.concatenate(key_parts)[:, None]


def joined(refs):
    return jnp.concatenate([ref[...] for ref in refs], axis=0)


def store_pieces(outs, total):
    rows = outs[0].shape[0]
    for place, ref in enumerate(outs):
        ref[...] = total[place * rows : (place + 1) * rows].astype(ref.dtype)


def probs_kernel(query_ref, grad_ref, query_ok_ref, key_ok_ref, *refs):
    key_refs, probs_out, value_outs = refs[:DOCB], refs[DOCB], refs[DOCB + 1 :]
    rows = query_ref.shape[0]
    group = query_ref.shape[1] // HD
    width = DOCB * rows
    scale = HD ** (-0.5)
    keys = joined(key_refs)
    key_at = lax.broadcasted_iota(jnp.int32, (width, rows), 0) - (width - rows)
    query_at = lax.broadcasted_iota(jnp.int32, (width, rows), 1)
    allowed = (key_ok_ref[...] > 0.0) & (key_at <= query_at)
    query_ok = query_ok_ref[...]
    value_sum = None
    for head in range(group):
        cols = slice(head * HD, (head + 1) * HD)
        g = grad_ref[:, cols] * query_ok
        scores = lax.dot_general(
            keys, query_ref[:, cols], (((1,), (1,)), ((), ())), preferred_element_type=F32
        )
        scores = jnp.where(allowed, scores * scale, masked_score)
        expd = jnp.exp(scores - jnp.max(scores, axis=0, keepdims=True))
        probs_low = (expd * (1.0 / jnp.sum(expd, axis=0, keepdims=True))).astype(BF16)
        probs_out[head] = probs_low
        value_part = jnp.dot(probs_low, g, preferred_element_type=F32)
        value_sum = value_part if value_sum is None else value_sum + value_part
    store_pieces(value_outs, value_sum)


def score_grad_kernel(query_ref, grad_ref, query_ok_ref, probs_ref, *refs):
    key_refs, value_refs = refs[:DOCB], refs[DOCB : 2 * DOCB]
    query_out, key_outs = refs[2 * DOCB], refs[2 * DOCB + 1 :]
    group = query_ref.shape[1] // HD
    scale = HD ** (-0.5)
    values = joined(value_refs)
    keys_turned = joined(key_refs).T
    query_ok = query_ok_ref[...]
    key_sum = None
    for head in range(group):
        cols = slice(head * HD, (head + 1) * HD)
        g = grad_ref[:, cols] * query_ok
        prob_grad = lax.dot_general(
            values, g, (((1,), (1,)), ((), ())), preferred_element_type=F32
        )
        probs = probs_ref[head].astype(F32)
        delta = jnp.sum(probs * prob_grad, axis=0, keepdims=True)
        score_grad = (probs * (prob_grad - delta) * scale).astype(BF16)
        query_grad = jnp.dot(keys_turned, score_grad, preferred_element_type=F32)
        query_out[:, cols] = query_grad.T.astype(BF16)
        key_part = jnp.dot(score_grad, query_ref[:, cols], preferred_element_type=F32)
        key_sum = key_part if key_sum is None else key_sum + key_part
    store_pieces(key_outs, key_sum)


def specs_of(query_rows, key_rows):
    rows, query_cols = query_rows.shape
    heads = key_rows.shape[1] // HD
    group = query_cols // HD // heads
    wide = pl.BlockSpec((rows, query_cols // heads), lambda h: (0, h))
    thin = pl.BlockSpec((rows, HD), lambda h: (0, h))
    query_mask = pl.BlockSpec((rows, 1), lambda h: (0, 0))
    key_mask = pl.BlockSpec((DOCB * rows, 1), lambda h: (0, 0))
    probs = pl.BlockSpec((group, DOCB * rows, rows), lambda h: (h, 0, 0))
    pieces = [
        jax.ShapeDtypeStruct(key_rows.shape, F32 if place == DOCB - 1 else BF16)
        for place in range(DOCB)
    ]
    options = dict(
        grid=(heads,),
        compiler_params=pltpu.CompilerParams(vmem_limit_bytes=48 * 2**20),
        cost_estimate=pl.CostEstimate(
            flops=20 * rows * DOCB * rows * query_cols, bytes_accessed=12 * 2**20, transcendentals=0
        ),
    )
    return wide, thin, query_mask, key_mask, probs, pieces, options


def window_probs(query_rows, grad_rows, query_ok, key_ok, keys):
    wide, thin, query_mask, key_mask, probs, pieces, options = specs_of(query_rows, keys[0])
    rows, query_cols = query_rows.shape
    outs = pl.pallas_call(
        probs_kernel,
        out_shape=[jax.ShapeDtypeStruct((query_cols // HD, DOCB * rows, rows), BF16)] + pieces,
        in_specs=[wide, wide, query_mask, key_mask] + [thin] * DOCB,
        out_specs=[probs] + [thin] * DOCB,
        **options,
    )(query_rows, grad_rows, query_ok, key_ok, *keys)
    return outs[0], outs[1:]


def window_score_grads(query_rows, grad_rows, query_ok, probs_low, keys, values):
    wide, thin, query_mask, _, probs, pieces, options = specs_of(query_rows, keys[0])
    outs = pl.pallas_call(
        score_grad_kernel,
        out_shape=[jax.ShapeDtypeStruct(query_rows.shape, BF16)] + pieces,
        in_specs=[wide, wide, query_mask, probs] + [thin] * (2 * DOCB),
        out_specs=[wide] + [thin] * DOCB,
        **options,
    )(query_rows, grad_rows, query_ok, probs_low, *keys, *values)
    return outs[0], outs[1:]


def window_of(block, core):
    two_back = from_behind(block, "node", 2)
    three_back = from_behind(block, "node", 3, parity=1)
    partner = swap(block, "node", 1)
    shared = swap(two_back, "node", 1)
    first = core == 0
    return [
        jnp.where(first, three_back, shared),
        two_back,
        jnp.where(first, shared, partner),
        block,
    ]


def sum_to_owner(pieces, core):
    three, two, one, own = pieces
    shared = swap(jnp.where(core == 0, one, three), "node", 1)
    near = from_behind(one, "node", -1, parity=1)
    far = from_behind(three, "node", -3, parity=0)
    back = from_behind((two.astype(F32) + shared.astype(F32)).astype(BF16), "node", -2)
    return own + near.astype(F32) + far.astype(F32) + back.astype(F32)


def gather_weight(weight, core):
    count, me = lax.axis_size("local"), lax.axis_index("local")
    rows = weight.shape[0]
    half = lax.dynamic_slice_in_dim(weight, core * (rows // 2), rows // 2, 0)
    pieces = [weight]
    for step in range(1, count):
        got = lax.ppermute(half, "local", [((i + step) % count, i) for i in range(count)])
        other = swap(got, "node", 1)
        pieces += [jnp.where(core == 0, got, other), jnp.where(core == 0, other, got)]
    around = jnp.concatenate(pieces + pieces, axis=0)
    return lax.dynamic_slice_in_dim(around, ((count - me) % count) * rows, count * rows, 0)


def halve(total, dim, axis, bit):
    mine = (lax.axis_index(axis) // bit) % 2
    pick = lambda i: lax.dynamic_index_in_dim(total, i, dim, keepdims=False)
    got = swap(pick(1 - mine).astype(BF16), axis, bit)
    return pick(mine) + got.astype(F32)


def scatter_weight_grad(x_rows, value_low, core):
    nodes, locals_ = lax.axis_size("node"), lax.axis_size("local")
    tokens, width = x_rows.shape
    kv_cols = value_low.shape[1]
    owner_rows = width // (nodes * locals_)
    split = x_rows.reshape(tokens, nodes // 2, 2, locals_ * owner_rows)
    contract_rows = (((0,), (0,)), ((), ()))

    def part(which):
        cols = lax.dynamic_index_in_dim(split, which, 2, keepdims=False)
        return lax.dot_general(
            cols.reshape(tokens, width // 2), value_low, contract_rows, preferred_element_type=F32
        )

    got = swap(part(1 - core).astype(BF16), "node", 1)
    total = part(core) + got.astype(F32)
    node_bits = [("node", 2**b) for b in range(1, nodes.bit_length() - 1)]
    local_bits = [("local", 2**b) for b in range(locals_.bit_length() - 1)]
    dims = node_bits[::-1] + local_bits[::-1]
    orders = (local_bits + node_bits, node_bits[:1] + local_bits + node_bits[1:])
    columns = kv_cols // 2
    done = []
    for which, order in enumerate(orders):
        piece = total[:, which * columns : (which + 1) * columns]
        piece = piece.reshape((2,) * len(dims) + (owner_rows, columns))
        left = list(dims)
        for step in order:
            piece = halve(piece, left.index(step), *step)
            left.remove(step)
        done.append(piece)
    return jnp.concatenate(done, axis=1)


def local(hidden, queries, saved_keys, grad_out, value_weight, doc_lengths, doc_order):
    block_index = lax.axis_index("node")
    core = block_index % 2
    x_rows = hidden[0]
    row_count = x_rows.shape[0]
    full_weight = gather_weight(value_weight, core)
    keys = window_of(saved_keys[0], core)
    layout = doc_layout(doc_lengths[0], doc_order[0], row_count)
    query_ok, key_ok = window_rows(block_index, layout, row_count)
    query_ok, key_ok = query_ok.astype(BF16), key_ok.astype(F32)
    probs_low, value_pieces = window_probs(queries[0], grad_out[0], query_ok, key_ok, keys)
    value_low = sum_to_owner(value_pieces, core).astype(BF16)
    weight_grad = scatter_weight_grad(x_rows, value_low, core)
    values = window_of(jnp.dot(x_rows, full_weight, preferred_element_type=F32).astype(BF16), core)
    query_grad, key_pieces = window_score_grads(
        queries[0], grad_out[0], query_ok, probs_low, keys, values
    )
    key_total = sum_to_owner(key_pieces, core)
    input_grad = lax.dot_general(
        value_low, full_weight, (((1,), (1,)), ((), ())), preferred_element_type=F32
    )
    return (
        query_grad[None],
        key_total.astype(BF16)[None],
        input_grad.astype(BF16)[None],
        weight_grad,
    )


def solution(mesh):
    placed = (
        P("local", "node", None),
        P("local", "node", None),
        P("local", "node", None),
        P("local", "node", None),
        P("local", None),
        P("local", None),
        P("local", None),
    )
    return jax.shard_map(
        local,
        mesh=mesh,
        in_specs=placed,
        out_specs=(
            P("local", "node", None),
            P("local", "node", None),
            P("local", "node", None),
            P(("node", "local"), None),
        ),
        check_vma=False,
    )
```

```python
import jax
import jax.numpy as jnp
from jax import lax
from jax.experimental import pallas as pl
from jax.experimental.pallas import tpu as pltpu
from jax.sharding import PartitionSpec as P

HD = 128
DOCB = 4
BF16 = jnp.bfloat16
F32 = jnp.float32

masked_score = -1e30


def from_behind(block, axis, distance, parity=None):
    devices = range(lax.axis_size(axis))
    route = [(i - distance, i) for i in devices if i - distance in devices]
    if parity is not None:
        route = [(a, b) for a, b in route if a % 2 == parity]
    return lax.ppermute(block, axis, route)


def swap(block, axis, bit):
    return lax.ppermute(block, axis, [(i, i ^ bit) for i in range(lax.axis_size(axis))])


def doc_layout(lengths_row, order_row, block_rows):
    slot_total = lengths_row.shape[0]
    slot_ids = jnp.arange(slot_total, dtype=jnp.int32)
    picked = order_row[:, None] == slot_ids[None, :]
    lens_ord = jnp.sum(jnp.where(picked, lengths_row[None, :], 0), axis=1)
    block_count = (lens_ord + block_rows - 1) // block_rows
    first_block = jnp.cumsum(block_count) - block_count
    return (lens_ord, block_count, first_block)


def block_info(block_index, lens_ord, block_count, first_block):
    member = (first_block <= block_index) & (block_index < first_block + block_count)
    has_doc = jnp.any(member)
    doc_start = jnp.sum(jnp.where(member, first_block, 0))
    length = jnp.sum(jnp.where(member, lens_ord, 0))
    return (jnp.where(has_doc, doc_start, -1), length)


def window_rows(block_index, layout, block_rows):
    doc_start, length = block_info(block_index, *layout)
    inside = jnp.arange(block_rows, dtype=jnp.int32)
    query_ok = (block_index - doc_start) * block_rows + inside < length
    key_parts = []
    for offset in range(DOCB - 1, -1, -1):
        other_block = block_index - offset
        other_start, _ = block_info(other_block, *layout)
        key_parts.append(
            (other_start == doc_start)
            & ((other_block - doc_start) * block_rows + inside < length)
        )
    return query_ok[:, None], jnp.concatenate(key_parts)[:, None]


def joined(refs):
    return jnp.concatenate([ref[...] for ref in refs], axis=0)


def store_pieces(outs, total):
    rows = outs[0].shape[0]
    for place, ref in enumerate(outs):
        ref[...] = total[place * rows : (place + 1) * rows].astype(ref.dtype)


def probs_kernel(query_ref, grad_ref, query_ok_ref, key_ok_ref, *refs):
    key_refs, probs_out, value_outs = refs[:DOCB], refs[DOCB], refs[DOCB + 1 :]
    rows = query_ref.shape[0]
    group = query_ref.shape[1] // HD
    width = DOCB * rows
    scale = HD ** (-0.5)
    keys = joined(key_refs)
    key_at = lax.broadcasted_iota(jnp.int32, (width, rows), 0) - (width - rows)
    query_at = lax.broadcasted_iota(jnp.int32, (width, rows), 1)
    allowed = (key_ok_ref[...] > 0.0) & (key_at <= query_at)
    query_ok = query_ok_ref[...]
    value_sum = None
    for head in range(group):
        cols = slice(head * HD, (head + 1) * HD)
        g = grad_ref[:, cols] * query_ok
        scores = lax.dot_general(
            keys, query_ref[:, cols], (((1,), (1,)), ((), ())), preferred_element_type=F32
        )
        scores = jnp.where(allowed, scores * scale, masked_score)
        expd = jnp.exp(scores - jnp.max(scores, axis=0, keepdims=True))
        probs_low = (expd * (1.0 / jnp.sum(expd, axis=0, keepdims=True))).astype(BF16)
        probs_out[head] = probs_low
        value_part = jnp.dot(probs_low, g, preferred_element_type=F32)
        value_sum = value_part if value_sum is None else value_sum + value_part
    store_pieces(value_outs, value_sum)


def score_grad_kernel(query_ref, grad_ref, query_ok_ref, probs_ref, *refs):
    key_refs, value_refs = refs[:DOCB], refs[DOCB : 2 * DOCB]
    query_out, key_outs = refs[2 * DOCB], refs[2 * DOCB + 1 :]
    group = query_ref.shape[1] // HD
    scale = HD ** (-0.5)
    values = joined(value_refs)
    keys_turned = joined(key_refs).T
    query_ok = query_ok_ref[...]
    key_sum = None
    for head in range(group):
        cols = slice(head * HD, (head + 1) * HD)
        g = grad_ref[:, cols] * query_ok
        prob_grad = lax.dot_general(
            values, g, (((1,), (1,)), ((), ())), preferred_element_type=F32
        )
        probs = probs_ref[head].astype(F32)
        delta = jnp.sum(probs * prob_grad, axis=0, keepdims=True)
        score_grad = (probs * (prob_grad - delta) * scale).astype(BF16)
        query_grad = jnp.dot(keys_turned, score_grad, preferred_element_type=F32)
        query_out[:, cols] = query_grad.T.astype(BF16)
        key_part = jnp.dot(score_grad, query_ref[:, cols], preferred_element_type=F32)
        key_sum = key_part if key_sum is None else key_sum + key_part
    store_pieces(key_outs, key_sum)


def specs_of(query_rows, key_rows):
    rows, query_cols = query_rows.shape
    heads = key_rows.shape[1] // HD
    group = query_cols // HD // heads
    wide = pl.BlockSpec((rows, query_cols // heads), lambda h: (0, h))
    thin = pl.BlockSpec((rows, HD), lambda h: (0, h))
    query_mask = pl.BlockSpec((rows, 1), lambda h: (0, 0))
    key_mask = pl.BlockSpec((DOCB * rows, 1), lambda h: (0, 0))
    probs = pl.BlockSpec((group, DOCB * rows, rows), lambda h: (h, 0, 0))
    pieces = [
        jax.ShapeDtypeStruct(key_rows.shape, F32 if place == DOCB - 1 else BF16)
        for place in range(DOCB)
    ]
    options = dict(
        grid=(heads,),
        compiler_params=pltpu.CompilerParams(vmem_limit_bytes=48 * 2**20),
        cost_estimate=pl.CostEstimate(
            flops=20 * rows * DOCB * rows * query_cols, bytes_accessed=12 * 2**20, transcendentals=0
        ),
    )
    return wide, thin, query_mask, key_mask, probs, pieces, options


def window_probs(query_rows, grad_rows, query_ok, key_ok, keys):
    wide, thin, query_mask, key_mask, probs, pieces, options = specs_of(query_rows, keys[0])
    rows, query_cols = query_rows.shape
    outs = pl.pallas_call(
        probs_kernel,
        out_shape=[jax.ShapeDtypeStruct((query_cols // HD, DOCB * rows, rows), BF16)] + pieces,
        in_specs=[wide, wide, query_mask, key_mask] + [thin] * DOCB,
        out_specs=[probs] + [thin] * DOCB,
        **options,
    )(query_rows, grad_rows, query_ok, key_ok, *keys)
    return outs[0], outs[1:]


def window_score_grads(query_rows, grad_rows, query_ok, probs_low, keys, values):
    wide, thin, query_mask, _, probs, pieces, options = specs_of(query_rows, keys[0])
    outs = pl.pallas_call(
        score_grad_kernel,
        out_shape=[jax.ShapeDtypeStruct(query_rows.shape, BF16)] + pieces,
        in_specs=[wide, wide, query_mask, probs] + [thin] * (2 * DOCB),
        out_specs=[wide] + [thin] * DOCB,
        **options,
    )(query_rows, grad_rows, query_ok, probs_low, *keys, *values)
    return outs[0], outs[1:]


def window_of(block, core):
    two_back = from_behind(block, "node", 2)
    three_back = from_behind(block, "node", 3, parity=1)
    partner = swap(block, "node", 1)
    shared = swap(two_back, "node", 1)
    first = core == 0
    return [
        jnp.where(first, three_back, shared),
        two_back,
        jnp.where(first, shared, partner),
        block,
    ]


def sum_to_owner(pieces, core):
    three, two, one, own = pieces
    shared = swap(jnp.where(core == 0, one, three), "node", 1)
    near = from_behind(one, "node", -1, parity=1)
    far = from_behind(three, "node", -3, parity=0)
    back = from_behind((two.astype(F32) + shared.astype(F32)).astype(BF16), "node", -2)
    return own + near.astype(F32) + far.astype(F32) + back.astype(F32)


def gather_weight(weight, core):
    count, me = lax.axis_size("local"), lax.axis_index("local")
    rows = weight.shape[0]
    half = lax.dynamic_slice_in_dim(weight, core * (rows // 2), rows // 2, 0)
    pieces = [weight]
    for step in range(1, count):
        got = lax.ppermute(half, "local", [((i + step) % count, i) for i in range(count)])
        other = swap(got, "node", 1)
        pieces += [jnp.where(core == 0, got, other), jnp.where(core == 0, other, got)]
    around = jnp.concatenate(pieces + pieces, axis=0)
    return lax.dynamic_slice_in_dim(around, ((count - me) % count) * rows, count * rows, 0)


def halves(total, dim, axis, bit):
    mine = (lax.axis_index(axis) // bit) % 2
    pick = lambda i: lax.dynamic_index_in_dim(total, i, dim, keepdims=False)
    return pick(mine), pick(1 - mine).astype(BF16)


def scatter_begin(x_rows, value_low, core):
    nodes, locals_ = lax.axis_size("node"), lax.axis_size("local")
    tokens, width = x_rows.shape
    kv_cols = value_low.shape[1]
    owner_rows = width // (nodes * locals_)
    split = x_rows.reshape(tokens, nodes // 2, 2, locals_ * owner_rows)
    contract_rows = (((0,), (0,)), ((), ()))

    def part(which):
        cols = lax.dynamic_index_in_dim(split, which, 2, keepdims=False)
        return lax.dot_general(
            cols.reshape(tokens, width // 2), value_low, contract_rows, preferred_element_type=F32
        )

    got = swap(part(1 - core).astype(BF16), "node", 1)
    total = part(core) + got.astype(F32)
    node_bits = [("node", 2**b) for b in range(1, nodes.bit_length() - 1)]
    local_bits = [("local", 2**b) for b in range(locals_.bit_length() - 1)]
    dims = node_bits[::-1] + local_bits[::-1]
    orders = (local_bits + node_bits, node_bits[:1] + local_bits + node_bits[1:])
    columns = kv_cols // 2
    begun = []
    for which, order in enumerate(orders):
        piece = total[:, which * columns : (which + 1) * columns]
        piece = piece.reshape((2,) * len(dims) + (owner_rows, columns))
        begun.append(halves(piece, dims.index(order[0]), *order[0]))
    return begun, orders, dims


def scatter_finish(begun, orders, dims):
    done = []
    for (keep, send), order in zip(begun, orders):
        left = list(dims)
        for place, step in enumerate(order):
            if place:
                keep, send = halves(piece, left.index(step), *step)
            left.remove(step)
            piece = keep + swap(send, *step).astype(F32)
        done.append(piece)
    return jnp.concatenate(done, axis=1)


def local(hidden, queries, saved_keys, grad_out, value_weight, doc_lengths, doc_order):
    block_index = lax.axis_index("node")
    core = block_index % 2
    x_rows = hidden[0]
    row_count = x_rows.shape[0]
    full_weight = gather_weight(value_weight, core)
    keys = window_of(saved_keys[0], core)
    layout = doc_layout(doc_lengths[0], doc_order[0], row_count)
    query_ok, key_ok = window_rows(block_index, layout, row_count)
    query_ok, key_ok = query_ok.astype(BF16), key_ok.astype(F32)
    probs_low, value_pieces = window_probs(queries[0], grad_out[0], query_ok, key_ok, keys)
    value_low = sum_to_owner(value_pieces, core).astype(BF16)
    begun, orders, dims = scatter_begin(x_rows, value_low, core)
    sends, query_ok = lax.optimization_barrier(([send for _, send in begun], query_ok))
    begun = [(keep, send) for (keep, _), send in zip(begun, sends)]
    weight_grad = scatter_finish(begun, orders, dims)
    values = window_of(jnp.dot(x_rows, full_weight, preferred_element_type=F32).astype(BF16), core)
    query_grad, key_pieces = window_score_grads(
        queries[0], grad_out[0], query_ok, probs_low, keys, values
    )
    key_total = sum_to_owner(key_pieces, core)
    input_grad = lax.dot_general(
        value_low, full_weight, (((1,), (1,)), ((), ())), preferred_element_type=F32
    )
    return (
        query_grad[None],
        key_total.astype(BF16)[None],
        input_grad.astype(BF16)[None],
        weight_grad,
    )


def solution(mesh):
    placed = (
        P("local", "node", None),
        P("local", "node", None),
        P("local", "node", None),
        P("local", "node", None),
        P("local", None),
        P("local", None),
        P("local", None),
    )
    return jax.shard_map(
        local,
        mesh=mesh,
        in_specs=placed,
        out_specs=(
            P("local", "node", None),
            P("local", "node", None),
            P("local", "node", None),
            P(("node", "local"), None),
        ),
        check_vma=False,
    )
```
